32 devices in a mesh: seq: 32 (over z, y, x, core), head: 1.
Axes of the slice: x: 2, y: 2, z: 4, core: 2. Of those that a mesh axis runs over, the one named last changes fastest.
Arguments:
- hidden: bfloat16 [4096, 1024], P('seq'), may hold values from -6 to 6
- query_weight: bfloat16 [1024, 512], P(None, 'head'), may hold values from -0.1875 to 0.1875
- key_weight: bfloat16 [1024, 512], P(None, 'head'), may hold values from -0.1875 to 0.1875
- values: bfloat16 [4096, 512], P('seq', 'head'), may hold values from -6 to 6
- grad_out: bfloat16 [4096, 512], P('seq', 'head'), may hold values from -6 to 6
- random_feats: float32 [8, 64, 256], P('head'), may hold values from -4 to 4
Outputs:
- grad_hidden: float32 [4096, 1024], P('seq')
- grad_values: bfloat16 [4096, 512], P('seq', 'head')
- grad_query_weight: float32 [1024, 512], P('seq', 'head')
- grad_key_weight: float32 [1024, 512], P('seq', 'head')
The draws below stay inside these ranges and needn't reach their ends.
All inputs are finite; a program needn't handle non-finite values.
Results may differ from the reference program's by a relative error of at most 0.0038.
Values sent between devices are 32-bit elements; how exact they have to be, the bound alone decides.
No kernel may reach another device: no remote copies, remote signals or barrier semaphores. Data moves between devices by JAX's collectives and lax.ppermute only.
A program may use at most 64 MiB of HBM per device.

```python
import jax
import jax.numpy as jnp
from jax import lax

D = 1024
HEADS = 8
DH = 64
M = 256
E = 512
S = 4096


def raised(drawn, own_key, source, target, blocks, factor):
    owner, partner = [(jnp.arange(drawn.shape[dim]) // (drawn.shape[dim] // blocks)).reshape([-1 if axis == dim else 1 for axis in range(drawn.ndim)]) for dim in (source, target)]
    chosen = jax.random.permutation(own_key, blocks)[partner]
    strong = (owner == chosen) | (owner == (partner + blocks // 2) % blocks)
    return jnp.where(strong, factor * drawn, drawn)


def steps_of(key, dims, split, least, top_value):
    def one(position, blocks):
        steps = jax.random.uniform(jax.random.fold_in(jax.random.fold_in(key, 6), position), (blocks,), jnp.float32, least / len(split), top_value / len(split))
        return jnp.repeat(jnp.exp(steps), dims[position] // blocks).reshape((-1,) + (1,) * (len(dims) - position - 1))

    gain = one(*split[0])
    for cut in split[1:]:
        gain = gain * one(*cut)
    return gain


def normal_values(own_key, extent, spread, reach, cuts=(), kind=jnp.bfloat16):
    result = jax.random.normal(own_key, extent, jnp.float32) * spread
    if len(cuts) > 0:
        result = steps_of(own_key, extent, cuts, -0.22, 0.18) * result
    return jnp.clip(result, min=-reach, max=reach).astype(kind)


def noise_with(key, dims, deviation, limit, split, heavy, dtype=jnp.bfloat16):
    entries = deviation * jax.random.normal(key, dims, jnp.float32)
    if split:
        entries = entries * steps_of(key, dims, split, -0.22, 0.18)
    return jnp.clip(raised(entries, jax.random.fold_in(key, 3), *heavy), -limit, limit).astype(dtype)


def setup_inputs(seed: int = 0) -> dict:
    key_of = jax.random.split(jax.random.key(seed), 7)
    return {
        "hidden": noise_with(key_of[0], (S, D), 1.0, 6.0, ((0, 32),), (0, 1, 32, 2.75)),
        "query_weight": normal_values(key_of[1], (D, E), D ** -0.5, 0.1875),
        "key_weight": normal_values(key_of[2], (D, E), D ** -0.5, 0.1875),
        "values": normal_values(key_of[3], (S, E), 1.0, 6.0, ((0, 32),)),
        "grad_out": normal_values(key_of[4], (S, E), 1.0, 6.0, ((0, 32),)),
        "random_feats": normal_values(key_of[5], (HEADS, DH, M), 1.0, 4.0, (), jnp.float32),
    }


HIGH = lax.Precision.HIGHEST

def features(rows, table):
    logits = jnp.dot(rows, table, precision=HIGH)
    half_norm = 0.5 * lax.optimization_barrier(jnp.sum(rows * rows, axis=1, keepdims=True))
    return jnp.exp(logits - half_norm) * M ** (-0.5)

def feature_grad(rows, feats, grads, table, feature_scale):
    weighted = feats * grads
    back = jnp.dot(weighted, table.T, precision=HIGH)
    return (back - rows * lax.optimization_barrier(jnp.sum(weighted, axis=1, keepdims=True))) * feature_scale

def one_head(packed):
    query_rows, key_rows, value_rows, upstream, table = packed
    feature_scale = DH ** (-0.25)
    query_feats = features(query_rows, table)
    key_feats = features(key_rows, table)
    value_state = jnp.dot(value_rows.T, key_feats, precision=HIGH)
    normalizer = lax.optimization_barrier(jnp.sum(key_feats, axis=0))
    numerator = jnp.dot(query_feats, value_state.T, precision=HIGH)
    denominator = jnp.dot(query_feats, normalizer, precision=HIGH)
    attended = numerator / denominator[:, None]
    grad_numer = upstream / denominator[:, None]
    grad_denom = -lax.optimization_barrier(jnp.sum(upstream * attended, axis=1)) / denominator
    grad_qfeat = jnp.dot(grad_numer, value_state, precision=HIGH) + grad_denom[:, None] * normalizer[None, :]
    grad_state = jnp.dot(grad_numer.T, query_feats, precision=HIGH)
    grad_normal = jnp.dot(grad_denom, query_feats, precision=HIGH)
    grad_kfeat = jnp.dot(value_rows, grad_state, precision=HIGH) + grad_normal[None, :]
    grad_value = jnp.dot(key_feats, grad_state.T, precision=HIGH)
    grad_query = feature_grad(query_rows, query_feats, grad_qfeat, table, feature_scale)
    grad_key = feature_grad(key_rows, key_feats, grad_kfeat, table, feature_scale)
    return (grad_query, grad_key, grad_value)

def split_heads(matrix):
    return matrix.reshape(S, HEADS, DH).transpose(1, 0, 2)

def join_heads(stacked):
    return stacked.transpose(1, 0, 2).reshape(S, E)

def reference(hidden, query_weight, key_weight, values, grad_out, random_feats):
    hidden_f = hidden.astype(jnp.float32)
    wq_f = query_weight.astype(jnp.float32)
    wk_f = key_weight.astype(jnp.float32)
    feature_scale = DH ** (-0.25)
    query_all = jnp.dot(hidden_f, wq_f, precision=HIGH) * feature_scale
    key_all = jnp.dot(hidden_f, wk_f, precision=HIGH) * feature_scale
    grad_query, grad_key, grad_value = lax.map(one_head, (split_heads(query_all), split_heads(key_all), split_heads(values.astype(jnp.float32)), split_heads(grad_out.astype(jnp.float32)), random_feats))
    dq_round = join_heads(grad_query).astype(jnp.bfloat16).astype(jnp.float32)
    dk_round = join_heads(grad_key).astype(jnp.bfloat16).astype(jnp.float32)
    grad_values = join_heads(grad_value).astype(jnp.bfloat16)
    grad_query_weight = jnp.dot(hidden_f.T, dq_round, precision=HIGH)
    grad_key_weight = jnp.dot(hidden_f.T, dk_round, precision=HIGH)
    grad_hidden = jnp.dot(dq_round, wq_f.T, precision=HIGH) + jnp.dot(dk_round, wk_f.T, precision=HIGH)
    return (grad_hidden, grad_values, grad_query_weight, grad_key_weight)
```

```python
import functools

import jax
import jax.numpy as jnp
from jax import lax
from jax.experimental import pallas as pl
from jax.experimental.pallas import tpu as pltpu
from jax.sharding import PartitionSpec as P

F32, BF16 = jnp.float32, jnp.bfloat16
NN = (((1,), (0,)), ((), ()))
NT = (((1,), (1,)), ((), ()))
TN = (((0,), (0,)), ((), ()))


def shape(*dims, dtype=F32):
    return jax.ShapeDtypeStruct(dims, dtype)


def split(value):
    high = value.astype(BF16)
    return high, (value - high.astype(F32)).astype(BF16)


def dot1(left, right, dims):
    return lax.dot_general(left, right, dims, preferred_element_type=F32)


def dot3(left, right, dims):
    lh, ll = left
    rh, rl = right
    return dot1(lh, rh, dims) + (dot1(lh, rl, dims) + dot1(ll, rh, dims))


def call(body, outs, *args, scalar=None):
    vmem = pl.BlockSpec(memory_space=pltpu.VMEM)
    specs = [vmem] * len(args)
    if scalar is not None:
        specs = [pl.BlockSpec(memory_space=pltpu.SMEM)] + specs
        args = (scalar,) + args
    return pl.pallas_call(
        body,
        out_shape=outs,
        in_specs=specs,
        out_specs=jax.tree.map(lambda _: vmem, outs),
    )(*args)


def project(hid, wq, wk, val, gout, packed, wide, *, dh, scale):
    rows = hid[...]
    wide[...] = rows.astype(F32)
    query = dot1(rows, wq[...], NN) * scale
    key = dot1(rows, wk[...], NN) * scale
    for h in range(packed.shape[0]):
        cols = slice(h * dh, (h + 1) * dh)
        packed[h, :, 0:dh] = query[:, cols]
        packed[h, :, dh : 2 * dh] = key[:, cols]
        packed[h, :, 2 * dh : 3 * dh] = val[:, cols].astype(F32)
        packed[h, :, 3 * dh : 4 * dh] = gout[:, cols].astype(F32)


def feats_of(rows, table):
    logits = dot3(split(rows), table, NN)
    half = 0.5 * jnp.sum(rows * rows, axis=1, keepdims=True)
    return jnp.exp(logits - half) * table[0].shape[1] ** (-0.5)


def key_state(inner, mine, feats, bfeat, state, *, dh):
    table = split(feats[inner[0]])
    total = jnp.zeros((state.shape[0], bfeat.shape[2]), F32)
    for t in range(mine.shape[0]):
        keys = mine[t, :, dh : 2 * dh]
        value = mine[t, :, 2 * dh : 3 * dh]
        feat = feats_of(keys, table)
        bfeat[t] = feat
        ones = jnp.ones((value.shape[0], state.shape[0] - dh), F32)
        rows = jnp.concatenate([value, ones], axis=1)
        total = total + dot3(split(rows), split(feat), TN)
    state[...] = total


def query_feats(inner, mine, feats, afeat, *, dh):
    table = split(feats[inner[0]])
    for t in range(mine.shape[0]):
        afeat[t] = feats_of(mine[t, :, 0:dh], table)


def query_state(mine, afeat, state, scaled, gstate, *, dh):
    pair = split(state[...])
    total = jnp.zeros(gstate.shape, F32)
    for t in range(mine.shape[0]):
        upstream = mine[t, :, 3 * dh : 4 * dh]
        feat = split(afeat[t])
        both = dot3(feat, pair, NT)
        inv = 1.0 / both[:, dh : dh + 1]
        gn = upstream * inv
        gd = -jnp.sum(gn * both[:, :dh], axis=1, keepdims=True) * inv
        zeros = jnp.zeros((gn.shape[0], gstate.shape[0] - dh - 1), F32)
        rows = jnp.concatenate([gn, gd, zeros], axis=1)
        scaled[t] = rows
        total = total + dot3(split(rows), feat, TN)
    gstate[...] = total


def row_grad(rows, feat, grads, table):
    weighted = feat * grads
    back = dot3(split(weighted), table, NT)
    return back - rows * jnp.sum(weighted, axis=1, keepdims=True)


def query_grad(inner, mine, feats, afeat, state, scaled, out, *, dh):
    table = split(feats[inner[0]])
    pair = split(state[...])
    for t in range(mine.shape[0]):
        grads = dot3(split(scaled[t]), pair, NN)
        out[t] = row_grad(mine[t, :, 0:dh], afeat[t], grads, table)


def key_grad(inner, mine, feats, bfeat, gstate, dq, out, back, *, dh):
    table = split(feats[inner[0]])
    pair = split(gstate[...])
    tok = mine.shape[1]
    for t in range(mine.shape[0]):
        value = mine[t, :, 2 * dh : 3 * dh]
        one = jnp.ones((tok, 1), F32)
        zeros = jnp.zeros((tok, gstate.shape[0] - dh - 1), F32)
        rows = jnp.concatenate([value, one, zeros], axis=1)
        grads = dot3(split(rows), pair, NN)
        feat = bfeat[t]
        dv = dot3(split(feat), pair, NT)[:, :dh]
        dk = row_grad(mine[t, :, dh : 2 * dh], feat, grads, table)
        out[t] = dk
        back[t, 0:tok, 0:dh] = dk
        back[t, 0:tok, dh : 2 * dh] = dv
        back[t, tok:, 0:dh] = dq[t, 0 : tok // 2]
        back[t, tok:, dh : 2 * dh] = dq[t, tok // 2 :]


def weight_part(inner, grads, *refs, scale):
    blocks, out = refs[:-1], refs[-1]
    outer, dh, width = out.shape
    total = jnp.zeros((dh, outer * width), F32)
    for j, block in enumerate(blocks):
        rows = (grads[inner[0] ^ j] * scale).astype(BF16)
        total = total + dot1(rows, block[...].astype(BF16), TN)
    for o in range(outer):
        out[o] = total[:, o * width : (o + 1) * width]


def finish_rows(back, wq, wk, grad_hidden, grad_values, *, scale):
    heads, rows, lanes = back.shape
    tok, dh = rows * 2 // 3, lanes // 2
    dqs, dks = [], []
    for h in range(heads):
        dks.append(back[h, 0:tok, 0:dh])
        dqs.append(jnp.concatenate([back[h, tok:, 0:dh], back[h, tok:, dh:]], axis=0))
        grad_values[:, h * dh : (h + 1) * dh] = back[h, 0:tok, dh:].astype(BF16)
    dq = (jnp.concatenate(dqs, axis=1) * scale).astype(BF16)
    dk = (jnp.concatenate(dks, axis=1) * scale).astype(BF16)
    grad_hidden[...] = dot1(dq, wq[...], NT) + dot1(dk, wk[...], NT)


def turn(keep_q, got_q, keep_k, got_k, out):
    dh = keep_q.shape[0]
    rows = jnp.concatenate([keep_q[...] + got_q[...], keep_k[...] + got_k[...]], axis=0)
    flat = rows.T
    count = out.shape[1]
    for i in range(out.shape[0]):
        out[i] = flat[i * count : (i + 1) * count]


def join(own, gq, gk):
    heads, _, lanes = own.shape
    dh = lanes // 2
    for h in range(heads):
        cols = slice(h * dh, (h + 1) * dh)
        gq[:, cols] = own[h, :, 0:dh]
        gk[:, cols] = own[h, :, dh:]


def make_shards(seq_count, head_count):
    def exchange(value, mask):
        return lax.ppermute(value, "seq", [(i, i ^ mask) for i in range(seq_count)])

    def shards(hidden, query_weight, key_weight, values, grad_out, random_feats):
        tok, width = hidden.shape
        group, dh, feats = random_feats.shape
        outer = seq_count // group
        assert outer * group == seq_count and outer & (outer - 1) == 0
        assert group & (group - 1) == 0 and width % seq_count == 0
        scale = dh ** (-0.25)
        padded = dh + 8
        groups = [[o * group + i for i in range(group)] for o in range(outer)]
        index = lax.axis_index("seq")
        inner = lax.rem(index, group)
        outer_index = index // group
        scalar = inner.reshape(1)

        def spread(value):
            return lax.all_to_all(
                value, "seq", 0, 0, axis_index_groups=groups, tiled=True
            )

        def plane_sum(value):
            step = 1
            while step < outer:
                value = value + exchange(value, step * group)
                step *= 2
            return value

        packed, wide = call(
            functools.partial(project, dh=dh, scale=scale),
            (shape(group, tok, 4 * dh), shape(tok, width)),
            hidden, query_weight, key_weight, values, grad_out,
        )
        mine = spread(packed)

        masks = [1 << b for b in range(1, group.bit_length() - 1)] + [1]

        def gather_step(blocks, mask):
            return blocks | {j ^ mask: exchange(item, mask) for j, item in blocks.items()}

        def after(blocks, value):
            return lax.optimization_barrier((blocks, value))

        blocks = gather_step({0: wide}, masks[0])

        bfeat, state = call(
            functools.partial(key_state, dh=dh),
            (shape(group, tok, feats), shape(padded, feats)),
            mine, random_feats, scalar=scalar,
        )
        blocks, state = after(blocks, state)
        for mask in masks[1:-1]:
            blocks = gather_step(blocks, mask)
        afeat = call(
            functools.partial(query_feats, dh=dh),
            shape(group, tok, feats),
            mine, random_feats, scalar=scalar,
        )
        state = plane_sum(state)
        scaled, gstate = call(
            functools.partial(query_state, dh=dh),
            (shape(group, tok, padded), shape(padded, feats)),
            mine, afeat, state,
        )
        blocks, gstate = after(blocks, gstate)
        for mask in masks[1:][-1:]:
            blocks = gather_step(blocks, mask)
        blocks = [blocks[j] for j in range(group)]
        dq = call(
            functools.partial(query_grad, dh=dh),
            shape(group, tok, dh),
            mine, random_feats, afeat, state, scaled, scalar=scalar,
        )

        def weight_of(grads):
            return call(
                functools.partial(weight_part, scale=scale),
                shape(outer, dh, width // outer),
                grads, *blocks, scalar=scalar,
            )

        def reduce_rows(part):
            step, got = 1, None
            while step < outer:
                bit = lax.rem(outer_index // step, 2)
                halves = part.reshape((part.shape[0] // 2, 2) + part.shape[1:])
                keep = lax.dynamic_index_in_dim(halves, bit, 1, keepdims=False)
                send = lax.dynamic_index_in_dim(halves, 1 - bit, 1, keepdims=False)
                got = exchange(send, step * group)
                step *= 2
                if step < outer:
                    part = keep + got
            return keep[0], got[0]

        part_q = reduce_rows(weight_of(dq))
        gstate = plane_sum(gstate)
        dk, back = call(
            functools.partial(key_grad, dh=dh),
            (shape(group, tok, dh), shape(group, tok + tok // 2, 2 * dh)),
            mine, random_feats, bfeat, gstate, dq, scalar=scalar,
        )
        part_k = reduce_rows(weight_of(dk))
        grad_hidden, grad_values = call(
            functools.partial(finish_rows, scale=scale),
            (shape(tok, width), shape(tok, group * dh, dtype=BF16)),
            spread(back), query_weight, key_weight,
        )
        if head_count > 1:
            grad_hidden = lax.psum(grad_hidden, "head")
        rows = width // seq_count
        grad_hidden, part_k = lax.optimization_barrier((grad_hidden, part_k))
        own = spread(call(turn, shape(group, rows, 2 * dh), *part_q, *part_k))
        grad_query_weight, grad_key_weight = call(
            join, (shape(rows, group * dh), shape(rows, group * dh)), own
        )
        return (grad_hidden, grad_values, grad_query_weight, grad_key_weight)

    return shards


def solution(mesh):
    placed = (
        P("seq", None),
        P(None, "head"),
        P(None, "head"),
        P("seq", "head"),
        P("seq", "head"),
        P("head", None, None),
    )
    return jax.shard_map(
        make_shards(mesh.shape["seq"], mesh.shape["head"]),
        mesh=mesh,
        in_specs=placed,
        out_specs=(P("seq", None), P("seq", "head"), P("seq", "head"), P("seq", "head")),
        check_vma=False,
    )
```

```python
import functools

import jax
import jax.numpy as jnp
from jax import lax
from jax.experimental import pallas as pl
from jax.experimental.pallas import tpu as pltpu
from jax.sharding import PartitionSpec as P


F32, BF16 = jnp.float32, jnp.bfloat16
NN = (((1,), (0,)), ((), ()))
NT = (((1,), (1,)), ((), ()))
TN = (((0,), (0,)), ((), ()))


def shape(*dims, dtype=F32):
    return jax.ShapeDtypeStruct(dims, dtype)


def split(value):
    high = value.astype(BF16)
    return high, (value - high.astype(F32)).astype(BF16)


def dot1(left, right, dims):
    return lax.dot_general(left, right, dims, preferred_element_type=F32)


def dot3(left, right, dims):
    lh, ll = left
    rh, rl = right
    return dot1(lh, rh, dims) + (dot1(lh, rl, dims) + dot1(ll, rh, dims))


def dot2(left, right, dims):
    rh, rl = right
    return dot1(left, rh, dims) + dot1(left, rl, dims)


CHUNK = 2
LIMIT = 24 << 20


def chunks(ref):
    step = min(CHUNK, ref.shape[0])
    return [slice(t, t + step) for t in range(0, ref.shape[0], step)]


def rows_of(ref, at, lanes=slice(None)):
    value = ref[at, :, lanes]
    return value.reshape(value.shape[0] * value.shape[1], value.shape[2])


def put(ref, at, value, lanes=slice(None)):
    ref[at, :, lanes] = value.reshape((at.stop - at.start, -1) + value.shape[1:])


def call(body, outs, *args, scratch=(), entry=(), final=False, loose=0):
    vmem = pl.BlockSpec(memory_space=pltpu.VMEM)
    specs = [vmem] * (len(entry) + len(args))
    args = [pltpu.with_memory_space_constraint(arg, pltpu.VMEM) for arg in args]
    args = list(entry) + args
    held = outs if final else jax.tree.map(lambda out: pltpu.VMEM(out.shape, out.dtype), outs)
    out_specs = jax.tree.map(lambda _: vmem, outs)
    if loose:
        held = tuple(pltpu.HBM(o.shape, o.dtype) for o in outs[:loose]) + held[loose:]
        out_specs = (pl.BlockSpec(memory_space=pl.ANY),) * loose + out_specs[loose:]
    return pl.pallas_call(
        body,
        out_shape=held,
        in_specs=specs,
        out_specs=out_specs,
        scratch_shapes=list(scratch),
        compiler_params=pltpu.CompilerParams(vmem_limit_bytes=LIMIT),
    )(*args)


def pack_pair(packed, first, second, dh):
    for h in range(packed.shape[0]):
        cols = slice(h * dh, (h + 1) * dh)
        packed[h, :, 0:dh] = first[:, cols]
        packed[h, :, dh : 2 * dh] = second[:, cols].astype(F32)


def project_key(hid, wk, val, packed, rows, weight, value, held, sems, *, dh, scale):
    step = 2 * dh
    count = weight.shape[0]
    loads = [
        pltpu.make_async_copy(hid, rows, sems.at[0]),
        pltpu.make_async_copy(val, value, sems.at[1]),
    ]
    for i in range(count):
        cols = wk.at[:, i * step : (i + 1) * step]
        loads.append(pltpu.make_async_copy(cols, weight.at[i], sems.at[2 + i]))
    for load in loads:
        load.start()
    loads[0].wait()
    loads[1].wait()
    stores = []
    for i in range(count):
        loads[2 + i].wait()
        key = dot1(rows[...], weight[i], NN) * scale
        items = value[:, i * step : (i + 1) * step].astype(F32)
        for j in range(2):
            held[2 * i + j, :, 0:dh] = key[:, j * dh : (j + 1) * dh]
            held[2 * i + j, :, dh:step] = items[:, j * dh : (j + 1) * dh]
        at = slice(2 * i, 2 * i + 2)
        stores.append(pltpu.make_async_copy(held.at[at], packed.at[at], sems.at[2 + count + i]))
        stores[-1].start()
    for store in stores:
        store.wait()


def project_query(hid, wq, gout, packed, *, dh, scale):
    pack_pair(packed, dot1(hid[...], wq[...], NN) * scale, gout, dh)


def widen(hid, wide_a, wide_b):
    half = wide_a.shape[0]
    wide_a[...] = hid[0:half].astype(F32)
    wide_b[...] = hid[half:].astype(F32)


def inner_of(group):
    return lax.rem(lax.axis_index("seq"), group)


def feats_of(rows, table):
    logits = dot3(split(rows), table, NN)
    half = 0.5 * jnp.sum(rows * rows, axis=1, keepdims=True)
    return jnp.exp(logits - half) * table[0].shape[1] ** (-0.5)


def key_state(feats, mine, bfeat, state, *, dh):
    table = split(feats[inner_of(feats.shape[0])])
    total = jnp.zeros((dh, state.shape[1]), F32)
    normal = jnp.zeros((1, state.shape[1]), F32)
    for at in chunks(mine):
        value = rows_of(mine, at, slice(dh, 2 * dh)).astype(BF16)
        feat = feats_of(rows_of(mine, at, slice(0, dh)), table)
        put(bfeat, at, feat)
        total = total + dot2(value, split(feat), TN)
        normal = normal + jnp.sum(feat, axis=0, keepdims=True)
    state[0:dh] = total
    state[dh:] = jnp.broadcast_to(normal, (state.shape[0] - dh, state.shape[1]))


def query_feats(feats, mine, afeat, *, dh):
    table = split(feats[inner_of(feats.shape[0])])
    for at in chunks(mine):
        put(afeat, at, feats_of(rows_of(mine, at, slice(0, dh)), table))


def query_state(mine, afeat, *refs, dh):
    parts, (state, scaled, gstate) = refs[:-3], refs[-3:]
    summed = sum(part[...] for part in parts)
    state[...] = summed
    pair = split(summed)
    total = jnp.zeros(gstate.shape, F32)
    for at in chunks(mine):
        upstream = rows_of(mine, at, slice(dh, 2 * dh))
        feat = split(rows_of(afeat, at))
        both = dot3(feat, pair, NT)
        inv = 1.0 / both[:, dh : dh + 1]
        gn = upstream * inv
        gd = -jnp.sum(gn * both[:, :dh], axis=1, keepdims=True) * inv
        zeros = jnp.zeros((gn.shape[0], gstate.shape[0] - dh - 1), F32)
        rows = jnp.concatenate([gn, gd, zeros], axis=1)
        put(scaled, at, rows)
        total = total + dot3(split(rows), feat, TN)
    gstate[...] = total


def row_grad(rows, feat, grads, table):
    weighted = feat * grads
    back = dot3(split(weighted), table, NT)
    return back - rows * jnp.sum(weighted, axis=1, keepdims=True)


def query_grad(feats, mine, afeat, state, scaled, out, *, dh):
    table = split(feats[inner_of(feats.shape[0])])
    pair = split(state[...])
    for at in chunks(mine):
        grads = dot3(split(rows_of(scaled, at)), pair, NN)
        put(out, at, row_grad(rows_of(mine, at, slice(0, dh)), rows_of(afeat, at), grads, table))


def emit_blocks(outer_index, total, held, outs):
    outer, _, width = held.shape
    for o in range(outer):
        held[o] = total[:, o * width : (o + 1) * width]
    for s, out in enumerate(outs):
        for i in range(out.shape[0]):
            out[i] = held[outer_index ^ (i * len(outs) + s)]


def gather_rows(*refs):
    blocks, rows_all = refs[:-1], refs[-1]
    group = len(blocks) // 2
    half = blocks[0].shape[0]
    inner = inner_of(group)
    for j in range(group):
        start = pl.multiple_of((inner ^ j) * 2 * half, 2 * half)
        for side in range(2):
            rows = blocks[2 * j + side][...].astype(BF16)
            rows_all[pl.ds(start + side * half, half), :] = rows


def key_grad(feats, mine, bfeat, dq, rows_all, *refs, dh, scale, count):
    parts, back, outs = refs[:count], refs[count], refs[count + 1 : -4]
    left, held, sent, sems = refs[-4:]
    group = mine.shape[0]
    copies = []
    table = split(feats[inner_of(feats.shape[0])])
    summed = sum(part[...] for part in parts)
    pair = split(summed[:dh])
    normal = summed[dh : dh + 1]
    tok = mine.shape[1]
    for at in chunks(mine):
        value = rows_of(mine, at, slice(dh, 2 * dh)).astype(BF16)
        grads = dot2(value, pair, NN) + normal
        feat = rows_of(bfeat, at)
        dv = dot3(split(feat), pair, NT)
        dk = row_grad(rows_of(mine, at, slice(0, dh)), feat, grads, table)
        both = jnp.concatenate([rows_of(dq, at), dk], axis=1) * scale
        left[at.start * tok : at.stop * tok, :] = both.astype(BF16)
        for t in range(at.start, at.stop):
            here = slice((t - at.start) * tok, (t - at.start + 1) * tok)
            sent[t, 0:tok, 0:dh] = dk[here]
            sent[t, 0:tok, dh : 2 * dh] = dv[here]
            sent[t, tok:, 0:dh] = dq[t, 0 : tok // 2]
            sent[t, tok:, dh : 2 * dh] = dq[t, tok // 2 :]
        copies.append(pltpu.make_async_copy(sent.at[at], back.at[at], sems.at[len(copies)]))
        copies[-1].start()
    outer_index = lax.axis_index("seq") // group
    emit_blocks(outer_index, dot1(left[...], rows_all[...], TN), held, outs)
    for copy in copies:
        copy.wait()


def finish_rows(wq, wk, back, grad_hidden, grad_values, *, scale):
    heads, rows, lanes = back.shape
    tok, dh = rows * 2 // 3, lanes // 2
    dqs, dks = [], []
    for h in range(heads):
        dks.append(back[h, 0:tok, 0:dh])
        dqs.append(jnp.concatenate([back[h, tok:, 0:dh], back[h, tok:, dh:]], axis=0))
        grad_values[:, h * dh : (h + 1) * dh] = back[h, 0:tok, dh:].astype(BF16)
    dq = (jnp.concatenate(dqs, axis=1) * scale).astype(BF16)
    dk = (jnp.concatenate(dks, axis=1) * scale).astype(BF16)
    grad_hidden[...] = dot1(dq, wq[...], NT) + dot1(dk, wk[...], NT)


def turn(*refs, count):
    parts, outs, flat = refs[:count], refs[count:-1], refs[-1]
    turned = sum(part[...] for part in parts).T
    group, rows, _ = flat.shape
    for i in range(group):
        flat[i] = turned[i * rows : (i + 1) * rows]
    inner = inner_of(group)
    for i, out in enumerate(outs):
        for j in range(out.shape[0]):
            out[j] = flat[inner ^ (2 * i + j)]


def join(*refs):
    firsts, last, (gq, gk), own = refs[:-4], refs[-4], refs[-3:-1], refs[-1]
    inner = inner_of(own.shape[0])
    for i, first in enumerate(firsts):
        own[inner ^ (2 * i)] = first[0]
        own[inner ^ (2 * i + 1)] = last[i]
    dh = own.shape[2] // 2
    for h in range(own.shape[0]):
        cols = slice(h * dh, (h + 1) * dh)
        gq[:, cols] = own[h, :, 0:dh]
        gk[:, cols] = own[h, :, dh:]


def make_shards(seq_count, head_count):
    def exchange(value, mask):
        return lax.ppermute(value, "seq", [(i, i ^ mask) for i in range(seq_count)])

    def inner_shards(hidden, query_weight, key_weight, values, grad_out, random_feats):
        tok, width = hidden.shape
        group, dh, feats = random_feats.shape
        outer = seq_count // group
        assert outer * group == seq_count and outer & (outer - 1) == 0
        assert group & (group - 1) == 0 and width % seq_count == 0
        scale = dh ** (-0.25)
        padded = dh + 8
        groups = [[o * group + i for i in range(group)] for o in range(outer)]
        radices = [2] * ((outer.bit_length() - 1) % 2) + [4] * ((outer.bit_length() - 1) // 2)

        def spread(value):
            return lax.all_to_all(
                value, "seq", 0, 0, axis_index_groups=groups, tiled=True
            )

        def plane_parts(value):
            parts, stride = [value], group
            for radix in radices:
                value = sum(parts)
                parts = [value] + [exchange(value, s * stride) for s in range(1, radix)]
                stride *= radix
            return parts

        def reduce_rows(sent):
            stride = group
            for i, radix in enumerate(radices):
                parts = [sent[0]] + [exchange(sent[s], s * stride) for s in range(1, radix)]
                stride *= radix
                if i + 1 < len(radices):
                    total = sum(parts)
                    total = total.reshape((-1, radices[i + 1]) + total.shape[1:])
                    sent = [total[:, s] for s in range(radices[i + 1])]
            return [part.reshape(part.shape[1:]) for part in parts]

        hbm = pl.BlockSpec(memory_space=pl.ANY)
        packed_kv = pl.pallas_call(
            functools.partial(project_key, dh=dh, scale=scale),
            out_shape=pltpu.HBM((group, tok, 2 * dh), F32),
            in_specs=[hbm] * 3,
            out_specs=hbm,
            scratch_shapes=[
                pltpu.VMEM((tok, width), BF16),
                pltpu.VMEM((group // 2, width, 2 * dh), BF16),
                pltpu.VMEM((tok, group * dh), BF16),
                pltpu.VMEM((group, tok, 2 * dh), F32),
                pltpu.SemaphoreType.DMA((2 + group,)),
            ],
            compiler_params=pltpu.CompilerParams(vmem_limit_bytes=LIMIT),
        )(*(pltpu.with_memory_space_constraint(x, pltpu.HBM) for x in (hidden, key_weight, values)))
        mine_kv = spread(packed_kv)
        packed_qg = call(
            functools.partial(project_query, dh=dh, scale=scale),
            shape(group, tok, 2 * dh),
            entry=(hidden, query_weight, grad_out),
        )
        mine_qg = spread(packed_qg)
        wide_a, wide_b = call(
            widen, (shape(tok // 2, width), shape(tok // 2, width)), entry=(hidden,)
        )

        bits = [1 << b for b in range(group.bit_length() - 1)]
        side_a = bits[1:] + bits[:1]
        side_b = bits[1:][::-1] + bits[:1]
        halves = [{0: wide_a}, {0: wide_b}]

        def gather_step(halves, k):
            return [
                side | {j ^ order[k]: exchange(item, order[k]) for j, item in side.items()}
                for side, order in zip(halves, (side_a, side_b))
            ]

        halves = gather_step(halves, 0)
        bfeat, state = call(
            functools.partial(key_state, dh=dh),
            (shape(group, tok, feats), shape(padded, feats)),
            mine_kv, entry=(random_feats,),
        )
        states = plane_parts(state)
        for k in range(1, len(bits) - 1):
            halves = gather_step(halves, k)
        afeat = call(
            functools.partial(query_feats, dh=dh),
            shape(group, tok, feats),
            mine_qg, entry=(random_feats,),
        )
        state, scaled, gstate = call(
            functools.partial(query_state, dh=dh),
            (shape(padded, feats), shape(group, tok, padded), shape(padded, feats)),
            mine_qg, afeat, *states,
        )
        gstates = plane_parts(gstate)
        dq = call(
            functools.partial(query_grad, dh=dh),
            shape(group, tok, dh),
            mine_qg, afeat, state, scaled, entry=(random_feats,),
        )
        halves = gather_step(halves, len(bits) - 1) if len(bits) > 1 else halves
        blocks = [side[j] for j in range(group) for side in halves]
        rows_all = call(gather_rows, shape(group * tok, width, dtype=BF16), *blocks)
        radix = radices[0]
        slabs = tuple(shape(outer // radix, 2 * dh, width // outer) for _ in range(radix))
        back, *sent = call(
            functools.partial(key_grad, dh=dh, scale=scale, count=len(gstates)),
            (shape(group, tok + tok // 2, 2 * dh),) + slabs,
            mine_kv, bfeat, dq, rows_all, *gstates, entry=(random_feats,), loose=1,
            scratch=[
                pltpu.VMEM((group * tok, 2 * dh), BF16),
                pltpu.VMEM((outer, 2 * dh, width // outer), F32),
                pltpu.VMEM((group, tok + tok // 2, 2 * dh), F32),
                pltpu.SemaphoreType.DMA((group,)),
            ],
        )
        parts = reduce_rows(sent)
        back = spread(back)
        grad_hidden, grad_values = call(
            functools.partial(finish_rows, scale=scale),
            (shape(tok, width), shape(tok, group * dh, dtype=BF16)),
            back, entry=(query_weight, key_weight), final=True,
        )
        if head_count > 1:
            grad_hidden = lax.psum(grad_hidden, "head")
        rows = width // seq_count
        mine, *others = call(
            functools.partial(turn, count=len(parts)),
            tuple(shape(2, rows, 2 * dh) for _ in range(group // 2)),
            *parts,
            scratch=[pltpu.VMEM((group, rows, 2 * dh), F32)],
        )
        firsts = [mine] + [exchange(item, 2 * i + 2) for i, item in enumerate(others)]
        last = exchange(jnp.stack([item[1] for item in firsts]), 1)
        grad_query_weight, grad_key_weight = call(
            join, (shape(rows, group * dh), shape(rows, group * dh)),
            *firsts, last, final=True,
            scratch=[pltpu.VMEM((group, rows, 2 * dh), F32)],
        )
        return (grad_hidden, grad_values, grad_query_weight, grad_key_weight)

    return inner_shards


def solution(mesh):
    placed = (
        P("seq", None),
        P(None, "head"),
        P(None, "head"),
        P("seq", "head"),
        P("seq", "head"),
        P("head", None, None),
    )
    return jax.shard_map(
        make_shards(mesh.shape["seq"], mesh.shape["head"]),
        mesh=mesh,
        in_specs=placed,
        out_specs=(P("seq", None), P("seq", "head"), P("seq", "head"), P("seq", "head")),
        check_vma=False,
    )
```

```python
import functools

import jax
import jax.numpy as jnp
from jax import lax
from jax.experimental import pallas as pl
from jax.experimental.pallas import tpu as pltpu
from jax.sharding import PartitionSpec as P


F32, BF16 = jnp.float32, jnp.bfloat16
NN = (((1,), (0,)), ((), ()))
NT = (((1,), (1,)), ((), ()))
TN = (((0,), (0,)), ((), ()))


def shape(*dims, dtype=F32):
    return jax.ShapeDtypeStruct(dims, dtype)


def split(value):
    high = value.astype(BF16)
    return high, (value - high.astype(F32)).astype(BF16)


def dot1(left, right, dims):
    return lax.dot_general(left, right, dims, preferred_element_type=F32)


def dot3(left, right, dims):
    lh, ll = left
    rh, rl = right
    return dot1(lh, rh, dims) + (dot1(lh, rl, dims) + dot1(ll, rh, dims))


def dot2(left, right, dims):
    rh, rl = right
    return dot1(left, rh, dims) + dot1(left, rl, dims)


CHUNK = 2
LIMIT = 12 << 20


def chunks(ref):
    step = min(CHUNK, ref.shape[0])
    return [slice(t, t + step) for t in range(0, ref.shape[0], step)]


def rows_of(ref, at, lanes=slice(None)):
    value = ref[at, :, lanes]
    return value.reshape(value.shape[0] * value.shape[1], value.shape[2])


def put(ref, at, value, lanes=slice(None)):
    ref[at, :, lanes] = value.reshape((at.stop - at.start, -1) + value.shape[1:])


def call(body, outs, *args, scratch=(), entry=(), final=False, loose=0):
    vmem = pl.BlockSpec(memory_space=pltpu.VMEM)
    specs = [vmem] * (len(entry) + len(args))
    args = [pltpu.with_memory_space_constraint(arg, pltpu.VMEM) for arg in args]
    args = list(entry) + args
    held = outs if final else jax.tree.map(lambda out: pltpu.VMEM(out.shape, out.dtype), outs)
    out_specs = jax.tree.map(lambda _: vmem, outs)
    if loose:
        held = tuple(pltpu.HBM(o.shape, o.dtype) for o in outs[:loose]) + held[loose:]
        out_specs = (pl.BlockSpec(memory_space=pl.ANY),) * loose + out_specs[loose:]
    return pl.pallas_call(
        body,
        out_shape=held,
        in_specs=specs,
        out_specs=out_specs,
        scratch_shapes=list(scratch),
        compiler_params=pltpu.CompilerParams(vmem_limit_bytes=LIMIT),
    )(*args)


def pack_pair(packed, first, second, dh):
    for h in range(packed.shape[0]):
        cols = slice(h * dh, (h + 1) * dh)
        packed[h, :, 0:dh] = first[:, cols]
        packed[h, :, dh : 2 * dh] = second[:, cols].astype(F32)


def project(hid, wk, val, wq, gout, *refs, dh, scale):
    outs, (packed, wide_a, wide_b) = refs[:-11], refs[-11:-8]
    rows, keys, queries, value, upstream, held, spare, sems = refs[-8:]
    count = (sems.shape[0] - 4) // 2
    step = keys.shape[0] // count
    loads = [
        pltpu.make_async_copy(hid, rows, sems.at[0]),
        pltpu.make_async_copy(val, value, sems.at[1]),
        pltpu.make_async_copy(gout, upstream, sems.at[2]),
    ]
    cuts = [slice(i * step, (i + 1) * step) for i in range(count)]
    for weight, kept in ((wk, keys), (wq, queries)):
        for at in cuts:
            loads.append(pltpu.make_async_copy(weight.at[at], kept.at[at], sems.at[len(loads)]))
    for load in loads:
        load.start()
    loads[0].wait()
    half = wide_a.shape[0]
    wide_a[...] = rows[0:half].astype(F32)
    wide_b[...] = rows[half:].astype(F32)

    def product(weight, first):
        total = jnp.zeros((rows.shape[0], weight.shape[1]), F32)
        for i, at in enumerate(cuts):
            loads[first + i].wait()
            total = total + dot1(rows[:, at], weight[at], NN)
        return total * scale

    key = product(keys, 3)
    loads[1].wait()
    pack_pair(held, key, value, dh)
    inner = inner_of(len(outs))
    for j, out in enumerate(outs):
        out[...] = held[inner ^ j]
    query = product(queries, 3 + count)
    loads[2].wait()
    pack_pair(spare, query, upstream, dh)
    store = pltpu.make_async_copy(spare, packed, sems.at[3 + 2 * count])
    store.start()
    store.wait()


def inner_of(group):
    return lax.rem(lax.axis_index("seq"), group)


def feats_of(rows, table):
    logits = dot3(split(rows), table, NN)
    half = 0.5 * jnp.sum(rows * rows, axis=1, keepdims=True)
    return jnp.exp(logits - half) * table[0].shape[1] ** (-0.5)


def pairs_of(refs):
    return [jnp.concatenate([a[...], b[...]], axis=0) for a, b in zip(refs[::2], refs[1::2])]


def key_state(feats, *refs, dh):
    blocks, state = refs[:-1], refs[-1]
    table = split(feats[inner_of(feats.shape[0])])
    total = jnp.zeros((dh, state.shape[1]), F32)
    normal = jnp.zeros((1, state.shape[1]), F32)
    for rows in pairs_of(blocks):
        feat = feats_of(rows[:, :dh], table)
        total = total + dot2(rows[:, dh:].astype(BF16), split(feat), TN)
        normal = normal + jnp.sum(feat, axis=0, keepdims=True)
    state[0:dh] = total
    state[dh:] = jnp.broadcast_to(normal, (state.shape[0] - dh, state.shape[1]))


def both_feats(feats, mine, *refs, dh):
    blocks, (afeat, bfeat) = refs[:-2], refs[-2:]
    table = split(feats[inner_of(feats.shape[0])])
    for at in chunks(mine):
        put(afeat, at, feats_of(rows_of(mine, at, slice(0, dh)), table))
    for i, rows in enumerate(pairs_of(blocks)):
        put(bfeat, slice(2 * i, 2 * i + 2), feats_of(rows[:, :dh], table))


def query_state(mine, afeat, *refs, dh):
    parts, (state, scaled, gstate) = refs[:-3], refs[-3:]
    summed = sum(part[...] for part in parts)
    state[...] = summed
    pair = split(summed)
    total = jnp.zeros(gstate.shape, F32)
    for at in chunks(mine):
        upstream = rows_of(mine, at, slice(dh, 2 * dh))
        feat = split(rows_of(afeat, at))
        both = dot3(feat, pair, NT)
        inv = 1.0 / both[:, dh : dh + 1]
        gn = upstream * inv
        gd = -jnp.sum(gn * both[:, :dh], axis=1, keepdims=True) * inv
        zeros = jnp.zeros((gn.shape[0], gstate.shape[0] - dh - 1), F32)
        rows = jnp.concatenate([gn, gd, zeros], axis=1)
        put(scaled, at, rows)
        total = total + dot3(split(rows), feat, TN)
    gstate[...] = total


def row_grad(rows, feat, grads, table):
    weighted = feat * grads
    back = dot3(split(weighted), table, NT)
    return back - rows * jnp.sum(weighted, axis=1, keepdims=True)


def query_grad(feats, mine, afeat, state, scaled, out, *, dh):
    table = split(feats[inner_of(feats.shape[0])])
    pair = split(state[...])
    for at in chunks(mine):
        grads = dot3(split(rows_of(scaled, at)), pair, NN)
        put(out, at, row_grad(rows_of(mine, at, slice(0, dh)), rows_of(afeat, at), grads, table))


def emit_blocks(outer_index, total, held, outs):
    outer, _, width = held.shape
    for o in range(outer):
        held[o] = total[:, o * width : (o + 1) * width]
    for s, out in enumerate(outs):
        for i in range(out.shape[0]):
            out[i] = held[outer_index ^ (i * len(outs) + s)]


def gather_rows(*refs):
    blocks, rows_all = refs[:-1], refs[-1]
    group = len(blocks) // 2
    half = blocks[0].shape[0]
    inner = inner_of(group)
    for j in range(group):
        start = pl.multiple_of((inner ^ j) * 2 * half, 2 * half)
        for side in range(2):
            rows = blocks[2 * j + side][...].astype(BF16)
            rows_all[pl.ds(start + side * half, half), :] = rows


def key_grad(feats, bfeat, dq, rows_all, *refs, dh, scale, count):
    parts, refs = refs[:count], refs[count:]
    group, tok, _ = bfeat.shape
    keys, outs = refs[:group], refs[group : 2 * group]
    sents, (left, held) = refs[2 * group : -2], refs[-2:]
    table = split(feats[inner_of(group)])
    summed = sum(part[...] for part in parts)
    pair = split(summed[:dh])
    normal = summed[dh : dh + 1]
    inner = inner_of(group)
    for i, rows in enumerate(pairs_of(keys)):
        grads = dot2(rows[:, dh:].astype(BF16), pair, NN) + normal
        feat = rows_of(bfeat, slice(2 * i, 2 * i + 2))
        dk = row_grad(rows[:, :dh], feat, grads, table)
        for side in range(2):
            j = 2 * i + side
            here = dk[side * tok : (side + 1) * tok]
            both = jnp.concatenate([dq[inner ^ j], here], axis=1) * scale
            start = pl.multiple_of((inner ^ j) * tok, tok)
            left[pl.ds(start, tok), :] = both.astype(BF16)
            outs[j][0:tok, 0:dh] = here
    emit_blocks(lax.axis_index("seq") // group, dot1(left[...], rows_all[...], TN), held, sents)
    for i in range(group // 2):
        dv = dot3(split(rows_of(bfeat, slice(2 * i, 2 * i + 2))), pair, NT)
        for side in range(2):
            j = 2 * i + side
            outs[j][0:tok, dh : 2 * dh] = dv[side * tok : (side + 1) * tok]
            outs[j][tok:, 0:dh] = dq[inner ^ j, 0 : tok // 2]
            outs[j][tok:, dh : 2 * dh] = dq[inner ^ j, tok // 2 :]


def finish_rows(wq, wk, *refs, scale):
    backs, (grad_hidden, grad_values, back) = refs[:-3], refs[-3:]
    inner = inner_of(len(backs))
    for j, item in enumerate(backs):
        back[inner ^ j] = item[...]
    heads, rows, lanes = back.shape
    tok, dh = rows * 2 // 3, lanes // 2
    dqs, dks = [], []
    for h in range(heads):
        dks.append(back[h, 0:tok, 0:dh])
        dqs.append(jnp.concatenate([back[h, tok:, 0:dh], back[h, tok:, dh:]], axis=0))
        grad_values[:, h * dh : (h + 1) * dh] = back[h, 0:tok, dh:].astype(BF16)
    dq = (jnp.concatenate(dqs, axis=1) * scale).astype(BF16)
    dk = (jnp.concatenate(dks, axis=1) * scale).astype(BF16)
    grad_hidden[...] = dot1(dq, wq[...], NT) + dot1(dk, wk[...], NT)


def load_weights(wq, wk, held_q, held_k, sems):
    copies = [
        pltpu.make_async_copy(wq, held_q, sems.at[0]),
        pltpu.make_async_copy(wk, held_k, sems.at[1]),
    ]
    for copy in copies:
        copy.start()
    for copy in copies:
        copy.wait()


def turn(*refs, count):
    parts, outs, flat = refs[:count], refs[count:-1], refs[-1]
    turned = sum(part[...] for part in parts).T
    group, rows, _ = flat.shape
    for i in range(group):
        flat[i] = turned[i * rows : (i + 1) * rows]
    inner = inner_of(group)
    for i, out in enumerate(outs):
        for j in range(out.shape[0]):
            out[j] = flat[inner ^ (2 * i + j)]


def join(*refs):
    firsts, last, (gq, gk), own = refs[:-4], refs[-4], refs[-3:-1], refs[-1]
    inner = inner_of(own.shape[0])
    for i, first in enumerate(firsts):
        own[inner ^ (2 * i)] = first[0]
        own[inner ^ (2 * i + 1)] = last[i]
    dh = own.shape[2] // 2
    for h in range(own.shape[0]):
        cols = slice(h * dh, (h + 1) * dh)
        gq[:, cols] = own[h, :, 0:dh]
        gk[:, cols] = own[h, :, dh:]


def make_shards(seq_count, head_count):
    def exchange(value, mask):
        return lax.ppermute(value, "seq", [(i, i ^ mask) for i in range(seq_count)])

    def inner_shards(hidden, query_weight, key_weight, values, grad_out, random_feats):
        tok, width = hidden.shape
        group, dh, feats = random_feats.shape
        outer = seq_count // group
        assert outer * group == seq_count and outer & (outer - 1) == 0
        assert group & (group - 1) == 0 and width % seq_count == 0
        scale = dh ** (-0.25)
        padded = dh + 8
        groups = [[o * group + i for i in range(group)] for o in range(outer)]
        radices = [2] * ((outer.bit_length() - 1) % 2) + [4] * ((outer.bit_length() - 1) // 2)

        def spread(value):
            return lax.all_to_all(
                value, "seq", 0, 0, axis_index_groups=groups, tiled=True
            )

        def plane_parts(value):
            parts, stride = [value], group
            for radix in radices:
                value = sum(parts)
                parts = [value] + [exchange(value, s * stride) for s in range(1, radix)]
                stride *= radix
            return parts

        def reduce_rows(sent):
            stride = group
            for i, radix in enumerate(radices):
                parts = [sent[0]] + [exchange(sent[s], s * stride) for s in range(1, radix)]
                stride *= radix
                if i + 1 < len(radices):
                    total = sum(parts)
                    total = total.reshape((-1, radices[i + 1]) + total.shape[1:])
                    sent = [total[:, s] for s in range(radices[i + 1])]
            return [part.reshape(part.shape[1:]) for part in parts]

        hbm = pl.BlockSpec(memory_space=pl.ANY)
        vmem = pl.BlockSpec(memory_space=pltpu.VMEM)
        entry = (hidden, key_weight, values, query_weight, grad_out)
        *packed, packed_qg, wide_a, wide_b = pl.pallas_call(
            functools.partial(project, dh=dh, scale=scale),
            out_shape=[pltpu.VMEM((tok, 2 * dh), F32) for _ in range(group)]
            + [pltpu.HBM((group, tok, 2 * dh), F32)]
            + [pltpu.VMEM((tok // 2, width), F32) for _ in range(2)],
            in_specs=[hbm] * 5,
            out_specs=[vmem] * group + [hbm] + [vmem] * 2,
            scratch_shapes=[
                pltpu.VMEM((tok, width), BF16),
                pltpu.VMEM((width, group * dh), BF16),
                pltpu.VMEM((width, group * dh), BF16),
                pltpu.VMEM((tok, group * dh), BF16),
                pltpu.VMEM((tok, group * dh), BF16),
                pltpu.VMEM((group, tok, 2 * dh), F32),
                pltpu.VMEM((group, tok, 2 * dh), F32),
                pltpu.SemaphoreType.DMA((12,)),
            ],
            compiler_params=pltpu.CompilerParams(vmem_limit_bytes=LIMIT),
        )(*(pltpu.with_memory_space_constraint(x, pltpu.HBM) for x in entry))
        mine_kv = [packed[0]] + [exchange(item, j) for j, item in enumerate(packed) if j]
        mine_qg = spread(packed_qg)

        bits = [1 << b for b in range(group.bit_length() - 1)]
        side_a = bits[1:] + bits[:1]
        side_b = bits[1:][::-1] + bits[:1]
        halves = [{0: wide_a}, {0: wide_b}]

        def gather_step(halves, k):
            return [
                side | {j ^ order[k]: exchange(item, order[k]) for j, item in side.items()}
                for side, order in zip(halves, (side_a, side_b))
            ]

        halves = gather_step(halves, 0)
        state = call(
            functools.partial(key_state, dh=dh),
            shape(padded, feats),
            *mine_kv, entry=(random_feats,),
        )
        states = plane_parts(state)
        for k in range(1, len(bits) - 1):
            halves = gather_step(halves, k)
        afeat, bfeat = call(
            functools.partial(both_feats, dh=dh),
            (shape(group, tok, feats), shape(group, tok, feats)),
            mine_qg, *mine_kv, entry=(random_feats,),
        )
        state, scaled, gstate = call(
            functools.partial(query_state, dh=dh),
            (shape(padded, feats), shape(group, tok, padded), shape(padded, feats)),
            mine_qg, afeat, *states,
        )
        gstates = plane_parts(gstate)
        dq = call(
            functools.partial(query_grad, dh=dh),
            shape(group, tok, dh),
            mine_qg, afeat, state, scaled, entry=(random_feats,),
        )
        halves = gather_step(halves, len(bits) - 1) if len(bits) > 1 else halves
        blocks = [side[j] for j in range(group) for side in halves]
        rows_all = call(gather_rows, shape(group * tok, width, dtype=BF16), *blocks)
        rows = width // seq_count
        radix = radices[0]
        results = call(
            functools.partial(key_grad, dh=dh, scale=scale, count=len(gstates)),
            tuple(shape(tok + tok // 2, 2 * dh) for _ in range(group))
            + tuple(shape(outer // radix, 2 * dh, width // outer) for _ in range(radix)),
            bfeat, dq, rows_all, *gstates, *mine_kv, entry=(random_feats,),
            scratch=[
                pltpu.VMEM((group * tok, 2 * dh), BF16),
                pltpu.VMEM((outer, 2 * dh, width // outer), F32),
            ],
        )
        backs, sent = list(results[:group]), list(results[group:])
        parts = reduce_rows(sent)
        backs = backs[:1] + [exchange(item, j) for j, item in enumerate(backs) if j]
        held = pl.pallas_call(
            load_weights,
            out_shape=[pltpu.VMEM(x.shape, BF16) for x in (query_weight, key_weight)],
            in_specs=[hbm] * 2,
            out_specs=[pl.BlockSpec(memory_space=pltpu.VMEM)] * 2,
            scratch_shapes=[pltpu.SemaphoreType.DMA((2,))],
        )(*(pltpu.with_memory_space_constraint(x, pltpu.HBM) for x in (query_weight, key_weight)))
        grad_hidden, grad_values = call(
            functools.partial(finish_rows, scale=scale),
            (shape(tok, width), shape(tok, group * dh, dtype=BF16)),
            *held, *backs, final=True,
            scratch=[pltpu.VMEM((group, tok + tok // 2, 2 * dh), F32)],
        )
        if head_count > 1:
            grad_hidden = lax.psum(grad_hidden, "head")
        mine, *others = call(
            functools.partial(turn, count=len(parts)),
            tuple(shape(2, rows, 2 * dh) for _ in range(group // 2)),
            *parts,
            scratch=[pltpu.VMEM((group, rows, 2 * dh), F32)],
        )
        firsts = [mine] + [exchange(item, 2 * i + 2) for i, item in enumerate(others)]
        last = exchange(jnp.stack([item[1] for item in firsts]), 1)
        grad_query_weight, grad_key_weight = call(
            join, (shape(rows, group * dh), shape(rows, group * dh)),
            *firsts, last, final=True,
            scratch=[pltpu.VMEM((group, rows, 2 * dh), F32)],
        )
        return (grad_hidden, grad_values, grad_query_weight, grad_key_weight)

    return inner_shards


def solution(mesh):
    placed = (
        P("seq", None),
        P(None, "head"),
        P(None, "head"),
        P("seq", "head"),
        P("seq", "head"),
        P("head", None, None),
    )
    return jax.shard_map(
        make_shards(mesh.shape["seq"], mesh.shape["head"]),
        mesh=mesh,
        in_specs=placed,
        out_specs=(P("seq", None), P("seq", "head"), P("seq", "head"), P("seq", "head")),
        check_vma=False,
    )
```

```python
import functools

import jax
import jax.numpy as jnp
from jax import lax
from jax.experimental import pallas as pl
from jax.experimental.pallas import tpu as pltpu
from jax.sharding import PartitionSpec as P


F32, BF16 = jnp.float32, jnp.bfloat16
NN = (((1,), (0,)), ((), ()))
NT = (((1,), (1,)), ((), ()))
TN = (((0,), (0,)), ((), ()))


def shape(*dims, dtype=F32):
    return jax.ShapeDtypeStruct(dims, dtype)


def split(value):
    high = value.astype(BF16)
    return high, (value - high.astype(F32)).astype(BF16)


def dot1(left, right, dims):
    return lax.dot_general(left, right, dims, preferred_element_type=F32)


def dot3(left, right, dims):
    lh, ll = left
    rh, rl = right
    return dot1(lh, rh, dims) + (dot1(lh, rl, dims) + dot1(ll, rh, dims))


def dot2(left, right, dims):
    rh, rl = right
    return dot1(left, rh, dims) + dot1(left, rl, dims)


LIMIT = 12 << 20


def rows_of(ref, at, lanes=slice(None)):
    value = ref[at, :, lanes]
    return value.reshape(value.shape[0] * value.shape[1], value.shape[2])


def put(ref, at, value, lanes=slice(None)):
    ref[at, :, lanes] = value.reshape((at.stop - at.start, -1) + value.shape[1:])


def call(body, outs, *args, scratch=(), entry=(), final=False, loose=0):
    vmem = pl.BlockSpec(memory_space=pltpu.VMEM)
    specs = [vmem] * (len(entry) + len(args))
    args = [pltpu.with_memory_space_constraint(arg, pltpu.VMEM) for arg in args]
    args = list(entry) + args
    held = outs if final else jax.tree.map(lambda out: pltpu.VMEM(out.shape, out.dtype), outs)
    out_specs = jax.tree.map(lambda _: vmem, outs)
    if loose:
        held = tuple(pltpu.HBM(o.shape, o.dtype) for o in outs[:loose]) + held[loose:]
        out_specs = (pl.BlockSpec(memory_space=pl.ANY),) * loose + out_specs[loose:]
    return pl.pallas_call(
        body,
        out_shape=held,
        in_specs=specs,
        out_specs=out_specs,
        scratch_shapes=list(scratch),
        compiler_params=pltpu.CompilerParams(vmem_limit_bytes=LIMIT),
    )(*args)


def pack_pair(packed, first, second, dh, at):
    for h in range(packed.shape[0]):
        cols = slice(h * dh, (h + 1) * dh)
        packed[h, :, at : at + dh] = first[:, cols]
        packed[h, :, at + dh : at + 2 * dh] = second[:, cols].astype(F32)


def project(hid, wk, val, wq, gout, *refs, dh, scale):
    outs, (wide_a, wide_b) = refs[:-9], refs[-9:-7]
    rows, keys, queries, value, upstream, held, sems = refs[-7:]
    count = (sems.shape[0] - 3) // 2
    step = keys.shape[0] // count
    loads = [
        pltpu.make_async_copy(hid, rows, sems.at[0]),
        pltpu.make_async_copy(val, value, sems.at[1]),
        pltpu.make_async_copy(gout, upstream, sems.at[2]),
    ]
    cuts = [slice(i * step, (i + 1) * step) for i in range(count)]
    for weight, kept in ((wk, keys), (wq, queries)):
        for at in cuts:
            loads.append(pltpu.make_async_copy(weight.at[at], kept.at[at], sems.at[len(loads)]))
    for load in loads:
        load.start()
    loads[0].wait()
    half = wide_a.shape[0]
    wide_a[...] = rows[0:half].astype(F32)
    wide_b[...] = rows[half:].astype(F32)

    def product(weight, first):
        total = jnp.zeros((rows.shape[0], weight.shape[1]), F32)
        for i, at in enumerate(cuts):
            loads[first + i].wait()
            total = total + dot1(rows[:, at], weight[at], NN)
        return total * scale

    key = product(keys, 3)
    loads[1].wait()
    pack_pair(held, key, value, dh, 0)
    query = product(queries, 3 + count)
    loads[2].wait()
    pack_pair(held, query, upstream, dh, 2 * dh)
    inner = inner_of(len(outs))
    for j, out in enumerate(outs):
        out[...] = held[inner ^ j]


def inner_of(group):
    return lax.rem(lax.axis_index("seq"), group)


def feats_of(rows, table):
    logits = dot3(split(rows), table, NN)
    half = 0.5 * jnp.sum(rows * rows, axis=1, keepdims=True)
    return jnp.exp(logits - half) * table[0].shape[1] ** (-0.5)


def pairs_of(refs):
    return [jnp.concatenate([a[...], b[...]], axis=0) for a, b in zip(refs[::2], refs[1::2])]


def key_state(feats, *refs, dh):
    blocks, state = refs[:-1], refs[-1]
    table = split(feats[inner_of(feats.shape[0])])
    total = jnp.zeros((dh, state.shape[1]), F32)
    normal = jnp.zeros((1, state.shape[1]), F32)
    for rows in pairs_of(blocks):
        feat = feats_of(rows[:, :dh], table)
        total = total + dot2(rows[:, dh : 2 * dh].astype(BF16), split(feat), TN)
        normal = normal + jnp.sum(feat, axis=0, keepdims=True)
    state[0:dh] = total
    state[dh:] = jnp.broadcast_to(normal, (state.shape[0] - dh, state.shape[1]))


def both_feats(feats, *refs, dh):
    blocks, (afeat, bfeat) = refs[:-2], refs[-2:]
    table = split(feats[inner_of(feats.shape[0])])
    for i, rows in enumerate(pairs_of(blocks)):
        at = slice(2 * i, 2 * i + 2)
        put(afeat, at, feats_of(rows[:, 2 * dh : 3 * dh], table))
        put(bfeat, at, feats_of(rows[:, :dh], table))


def query_state(afeat, *refs, dh):
    group = afeat.shape[0]
    blocks, parts, (state, scaled, gstate) = refs[:group], refs[group:-3], refs[-3:]
    summed = sum(part[...] for part in parts)
    state[...] = summed
    pair = split(summed)
    total = jnp.zeros(gstate.shape, F32)
    for i, block in enumerate(pairs_of(blocks)):
        at = slice(2 * i, 2 * i + 2)
        upstream = block[:, 3 * dh :]
        feat = split(rows_of(afeat, at))
        both = dot3(feat, pair, NT)
        inv = 1.0 / both[:, dh : dh + 1]
        gn = upstream * inv
        gd = -jnp.sum(gn * both[:, :dh], axis=1, keepdims=True) * inv
        zeros = jnp.zeros((gn.shape[0], gstate.shape[0] - dh - 1), F32)
        rows = jnp.concatenate([gn, gd, zeros], axis=1)
        put(scaled, at, rows)
        total = total + dot3(split(rows), feat, TN)
    gstate[...] = total


def row_grad(rows, feat, grads, table):
    weighted = feat * grads
    back = dot3(split(weighted), table, NT)
    return back - rows * jnp.sum(weighted, axis=1, keepdims=True)


def query_grad(feats, afeat, state, scaled, *refs, dh):
    blocks, out = refs[:-1], refs[-1]
    table = split(feats[inner_of(feats.shape[0])])
    pair = split(state[...])
    for i, rows in enumerate(pairs_of(blocks)):
        at = slice(2 * i, 2 * i + 2)
        grads = dot3(split(rows_of(scaled, at)), pair, NN)
        put(out, at, row_grad(rows[:, 2 * dh : 3 * dh], rows_of(afeat, at), grads, table))


def emit_blocks(outer_index, total, held, outs):
    outer, _, width = held.shape
    for o in range(outer):
        held[o] = total[:, o * width : (o + 1) * width]
    for s, out in enumerate(outs):
        for i in range(out.shape[0]):
            out[i] = held[outer_index ^ (i * len(outs) + s)]


def gather_rows(*refs):
    blocks, rows_all = refs[:-1], refs[-1]
    group = len(blocks) // 2
    half = blocks[0].shape[0]
    inner = inner_of(group)
    for j in range(group):
        start = pl.multiple_of((inner ^ j) * 2 * half, 2 * half)
        for side in range(2):
            rows = blocks[2 * j + side][...].astype(BF16)
            rows_all[pl.ds(start + side * half, half), :] = rows


def key_grad(feats, bfeat, dq, rows_all, *refs, dh, scale, count):
    parts, refs = refs[:count], refs[count:]
    group, tok, _ = bfeat.shape
    keys, out, sents, (left, held) = refs[:group], refs[group], refs[group + 1 : -2], refs[-2:]
    table = split(feats[inner_of(group)])
    summed = sum(part[...] for part in parts)
    pair = split(summed[:dh])
    normal = summed[dh : dh + 1]
    inner = inner_of(group)
    for i, rows in enumerate(pairs_of(keys)):
        at = slice(2 * i, 2 * i + 2)
        grads = dot2(rows[:, dh : 2 * dh].astype(BF16), pair, NN) + normal
        dk = row_grad(rows[:, :dh], rows_of(bfeat, at), grads, table)
        put(out, at, dk)
        both = (jnp.concatenate([rows_of(dq, at), dk], axis=1) * scale).astype(BF16)
        for side in range(2):
            start = pl.multiple_of((inner ^ (2 * i + side)) * tok, tok)
            left[pl.ds(start, tok), :] = both[side * tok : (side + 1) * tok]
    emit_blocks(lax.axis_index("seq") // group, dot1(left[...], rows_all[...], TN), held, sents)


def back_rows(bfeat, dq, dk, *refs, dh, count):
    parts, outs = refs[:count], refs[count:]
    group, tok, _ = bfeat.shape
    pair = split(sum(part[0:dh] for part in parts))
    for i in range(group // 2):
        dv = dot3(split(rows_of(bfeat, slice(2 * i, 2 * i + 2))), pair, NT)
        for side in range(2):
            j = 2 * i + side
            outs[j][0:tok, 0:dh] = dk[j]
            outs[j][0:tok, dh : 2 * dh] = dv[side * tok : (side + 1) * tok]
            outs[j][tok:, 0:dh] = dq[j, 0 : tok // 2]
            outs[j][tok:, dh : 2 * dh] = dq[j, tok // 2 :]


def finish_rows(wq, wk, *refs, scale):
    backs, (grad_hidden, grad_values, back) = refs[:-3], refs[-3:]
    inner = inner_of(len(backs))
    for j, item in enumerate(backs):
        back[inner ^ j] = item[...]
    heads, rows, lanes = back.shape
    tok, dh = rows * 2 // 3, lanes // 2
    dqs, dks = [], []
    for h in range(heads):
        dks.append(back[h, 0:tok, 0:dh])
        dqs.append(jnp.concatenate([back[h, tok:, 0:dh], back[h, tok:, dh:]], axis=0))
        grad_values[:, h * dh : (h + 1) * dh] = back[h, 0:tok, dh:].astype(BF16)
    dq = (jnp.concatenate(dqs, axis=1) * scale).astype(BF16)
    dk = (jnp.concatenate(dks, axis=1) * scale).astype(BF16)
    grad_hidden[...] = dot1(dq, wq[...], NT) + dot1(dk, wk[...], NT)


def load_weights(wq, wk, held_q, held_k, sems):
    copies = [
        pltpu.make_async_copy(wq, held_q, sems.at[0]),
        pltpu.make_async_copy(wk, held_k, sems.at[1]),
    ]
    for copy in copies:
        copy.start()
    for copy in copies:
        copy.wait()


def turn(*refs, count):
    parts, outs, flat = refs[:count], refs[count:-1], refs[-1]
    turned = sum(part[...] for part in parts).T
    group, rows, _ = flat.shape
    for i in range(group):
        flat[i] = turned[i * rows : (i + 1) * rows]
    inner = inner_of(group)
    for i, out in enumerate(outs):
        for j in range(out.shape[0]):
            out[j] = flat[inner ^ (2 * i + j)]


def join(*refs):
    firsts, last, (gq, gk), own = refs[:-4], refs[-4], refs[-3:-1], refs[-1]
    inner = inner_of(own.shape[0])
    for i, first in enumerate(firsts):
        own[inner ^ (2 * i)] = first[0]
        own[inner ^ (2 * i + 1)] = last[i]
    dh = own.shape[2] // 2
    for h in range(own.shape[0]):
        cols = slice(h * dh, (h + 1) * dh)
        gq[:, cols] = own[h, :, 0:dh]
        gk[:, cols] = own[h, :, dh:]


def make_shards(seq_count, head_count):
    def exchange(value, mask):
        return lax.ppermute(value, "seq", [(i, i ^ mask) for i in range(seq_count)])

    def inner_shards(hidden, query_weight, key_weight, values, grad_out, random_feats):
        tok, width = hidden.shape
        group, dh, feats = random_feats.shape
        outer = seq_count // group
        assert outer * group == seq_count and outer & (outer - 1) == 0
        assert group & (group - 1) == 0 and width % seq_count == 0
        scale = dh ** (-0.25)
        padded = dh + 8
        radices = [2] * ((outer.bit_length() - 1) % 2) + [4] * ((outer.bit_length() - 1) // 2)

        def plane_parts(value):
            parts, stride = [value], group
            for radix in radices:
                value = sum(parts)
                parts = [value] + [exchange(value, s * stride) for s in range(1, radix)]
                stride *= radix
            return parts

        def reduce_rows(sent):
            stride = group
            for i, radix in enumerate(radices):
                parts = [sent[0]] + [exchange(sent[s], s * stride) for s in range(1, radix)]
                stride *= radix
                if i + 1 < len(radices):
                    total = sum(parts)
                    total = total.reshape((-1, radices[i + 1]) + total.shape[1:])
                    sent = [total[:, s] for s in range(radices[i + 1])]
            return [part.reshape(part.shape[1:]) for part in parts]

        hbm = pl.BlockSpec(memory_space=pl.ANY)
        vmem = pl.BlockSpec(memory_space=pltpu.VMEM)
        entry = (hidden, key_weight, values, query_weight, grad_out)
        *packed, wide_a, wide_b = pl.pallas_call(
            functools.partial(project, dh=dh, scale=scale),
            out_shape=[pltpu.VMEM((tok, 4 * dh), F32) for _ in range(group)]
            + [pltpu.VMEM((tok // 2, width), F32) for _ in range(2)],
            in_specs=[hbm] * 5,
            out_specs=[vmem] * (group + 2),
            scratch_shapes=[
                pltpu.VMEM((tok, width), BF16),
                pltpu.VMEM((width, group * dh), BF16),
                pltpu.VMEM((width, group * dh), BF16),
                pltpu.VMEM((tok, group * dh), BF16),
                pltpu.VMEM((tok, group * dh), BF16),
                pltpu.VMEM((group, tok, 4 * dh), F32),
                pltpu.SemaphoreType.DMA((11,)),
            ],
            compiler_params=pltpu.CompilerParams(vmem_limit_bytes=LIMIT),
        )(*(pltpu.with_memory_space_constraint(x, pltpu.HBM) for x in entry))
        mine = [packed[0]] + [exchange(item, j) for j, item in enumerate(packed) if j]

        bits = [1 << b for b in range(group.bit_length() - 1)]
        side_a = bits[1:] + bits[:1]
        side_b = bits[1:][::-1] + bits[:1]
        halves = [{0: wide_a}, {0: wide_b}]

        def gather_step(halves, k):
            return [
                side | {j ^ order[k]: exchange(item, order[k]) for j, item in side.items()}
                for side, order in zip(halves, (side_a, side_b))
            ]

        halves = gather_step(halves, 0)
        state = call(
            functools.partial(key_state, dh=dh),
            shape(padded, feats),
            *mine, entry=(random_feats,),
        )
        states = plane_parts(state)
        for k in range(1, len(bits) - 1):
            halves = gather_step(halves, k)
        afeat, bfeat = call(
            functools.partial(both_feats, dh=dh),
            (shape(group, tok, feats), shape(group, tok, feats)),
            *mine, entry=(random_feats,),
        )
        state, scaled, gstate = call(
            functools.partial(query_state, dh=dh),
            (shape(padded, feats), shape(group, tok, padded), shape(padded, feats)),
            afeat, *mine, *states,
        )
        gstates = plane_parts(gstate)
        dq = call(
            functools.partial(query_grad, dh=dh),
            shape(group, tok, dh),
            afeat, state, scaled, *mine, entry=(random_feats,),
        )
        halves = gather_step(halves, len(bits) - 1) if len(bits) > 1 else halves
        blocks = [side[j] for j in range(group) for side in halves]
        rows_all = call(gather_rows, shape(group * tok, width, dtype=BF16), *blocks)
        rows = width // seq_count
        radix = radices[0]
        dk, *sent = call(
            functools.partial(key_grad, dh=dh, scale=scale, count=len(gstates)),
            (shape(group, tok, dh),)
            + tuple(shape(outer // radix, 2 * dh, width // outer) for _ in range(radix)),
            bfeat, dq, rows_all, *gstates, *mine, entry=(random_feats,),
            scratch=[
                pltpu.VMEM((group * tok, 2 * dh), BF16),
                pltpu.VMEM((outer, 2 * dh, width // outer), F32),
            ],
        )
        parts = reduce_rows(sent)
        backs = call(
            functools.partial(back_rows, dh=dh, count=len(gstates)),
            tuple(shape(tok + tok // 2, 2 * dh) for _ in range(group)),
            bfeat, dq, dk, *gstates,
        )
        backs = [backs[0]] + [exchange(item, j) for j, item in enumerate(backs) if j]
        held = pl.pallas_call(
            load_weights,
            out_shape=[pltpu.VMEM(x.shape, BF16) for x in (query_weight, key_weight)],
            in_specs=[hbm] * 2,
            out_specs=[pl.BlockSpec(memory_space=pltpu.VMEM)] * 2,
            scratch_shapes=[pltpu.SemaphoreType.DMA((2,))],
        )(*(pltpu.with_memory_space_constraint(x, pltpu.HBM) for x in (query_weight, key_weight)))
        grad_hidden, grad_values = call(
            functools.partial(finish_rows, scale=scale),
            (shape(tok, width), shape(tok, group * dh, dtype=BF16)),
            *held, *backs, final=True,
            scratch=[pltpu.VMEM((group, tok + tok // 2, 2 * dh), F32)],
        )
        if head_count > 1:
            grad_hidden = lax.psum(grad_hidden, "head")
        mine, *others = call(
            functools.partial(turn, count=len(parts)),
            tuple(shape(2, rows, 2 * dh) for _ in range(group // 2)),
            *parts,
            scratch=[pltpu.VMEM((group, rows, 2 * dh), F32)],
        )
        firsts = [mine] + [exchange(item, 2 * i + 2) for i, item in enumerate(others)]
        last = exchange(jnp.stack([item[1] for item in firsts]), 1)
        grad_query_weight, grad_key_weight = call(
            join, (shape(rows, group * dh), shape(rows, group * dh)),
            *firsts, last, final=True,
            scratch=[pltpu.VMEM((group, rows, 2 * dh), F32)],
        )
        return (grad_hidden, grad_values, grad_query_weight, grad_key_weight)

    return inner_shards


def solution(mesh):
    placed = (
        P("seq", None),
        P(None, "head"),
        P(None, "head"),
        P("seq", "head"),
        P("seq", "head"),
        P("head", None, None),
    )
    return jax.shard_map(
        make_shards(mesh.shape["seq"], mesh.shape["head"]),
        mesh=mesh,
        in_specs=placed,
        out_specs=(P("seq", None), P("seq", "head"), P("seq", "head"), P("seq", "head")),
        check_vma=False,
    )
```

```python
import functools

import jax
import jax.numpy as jnp
from jax import lax
from jax.experimental import pallas as pl
from jax.experimental.pallas import tpu as pltpu
from jax.sharding import PartitionSpec as P


F32, BF16 = jnp.float32, jnp.bfloat16
NN = (((1,), (0,)), ((), ()))
NT = (((1,), (1,)), ((), ()))
TN = (((0,), (0,)), ((), ()))


def shape(*dims, dtype=F32):
    return jax.ShapeDtypeStruct(dims, dtype)


def split(value):
    high = value.astype(BF16)
    return high, (value - high.astype(F32)).astype(BF16)


def dot1(left, right, dims):
    return lax.dot_general(left, right, dims, preferred_element_type=F32)


def dot3(left, right, dims):
    lh, ll = left
    rh, rl = right
    return dot1(lh, rh, dims) + (dot1(lh, rl, dims) + dot1(ll, rh, dims))


def dot2(left, right, dims):
    rh, rl = right
    return dot1(left, rh, dims) + dot1(left, rl, dims)


LIMIT = 12 << 20


def rows_of(ref, at, lanes=slice(None)):
    value = ref[at, :, lanes]
    return value.reshape(value.shape[0] * value.shape[1], value.shape[2])


def put(ref, at, value, lanes=slice(None)):
    ref[at, :, lanes] = value.reshape((at.stop - at.start, -1) + value.shape[1:])


def call(body, outs, *args, scratch=(), entry=(), final=False, loose=0):
    vmem = pl.BlockSpec(memory_space=pltpu.VMEM)
    specs = [vmem] * (len(entry) + len(args))
    args = [pltpu.with_memory_space_constraint(arg, pltpu.VMEM) for arg in args]
    args = list(entry) + args
    held = outs if final else jax.tree.map(lambda out: pltpu.VMEM(out.shape, out.dtype), outs)
    out_specs = jax.tree.map(lambda _: vmem, outs)
    if loose:
        held = tuple(pltpu.HBM(o.shape, o.dtype) for o in outs[:loose]) + held[loose:]
        out_specs = (pl.BlockSpec(memory_space=pl.ANY),) * loose + out_specs[loose:]
    return pl.pallas_call(
        body,
        out_shape=held,
        in_specs=specs,
        out_specs=out_specs,
        scratch_shapes=list(scratch),
        compiler_params=pltpu.CompilerParams(vmem_limit_bytes=LIMIT),
    )(*args)


def pack_pair(packed, first, second, dh, at):
    for h in range(packed.shape[0]):
        cols = slice(h * dh, (h + 1) * dh)
        packed[h, :, at : at + dh] = first[:, cols]
        packed[h, :, at + dh : at + 2 * dh] = second[:, cols].astype(F32)


def project(hid, wk, val, wq, gout, *refs, dh, scale):
    outs, (wide_a, wide_b) = refs[:-9], refs[-9:-7]
    rows, keys, queries, value, upstream, held, sems = refs[-7:]
    count = (sems.shape[0] - 3) // 2
    step = keys.shape[0] // count
    loads = [
        pltpu.make_async_copy(hid, rows, sems.at[0]),
        pltpu.make_async_copy(val, value, sems.at[1]),
        pltpu.make_async_copy(gout, upstream, sems.at[2]),
    ]
    cuts = [slice(i * step, (i + 1) * step) for i in range(count)]
    for weight, kept in ((wk, keys), (wq, queries)):
        for at in cuts:
            loads.append(pltpu.make_async_copy(weight.at[at], kept.at[at], sems.at[len(loads)]))
    for load in loads:
        load.start()
    loads[0].wait()
    half = wide_a.shape[0]
    wide_a[...] = rows[0:half].astype(F32)
    wide_b[...] = rows[half:].astype(F32)

    def product(weight, first):
        total = jnp.zeros((rows.shape[0], weight.shape[1]), F32)
        for i, at in enumerate(cuts):
            loads[first + i].wait()
            total = total + dot1(rows[:, at], weight[at], NN)
        return total * scale

    key = product(keys, 3)
    loads[1].wait()
    pack_pair(held, key, value, dh, 0)
    query = product(queries, 3 + count)
    loads[2].wait()
    pack_pair(held, query, upstream, dh, 2 * dh)
    inner = inner_of(len(outs))
    for j, out in enumerate(outs):
        out[...] = held[inner ^ j]


def inner_of(group):
    return lax.rem(lax.axis_index("seq"), group)


def feats_of(rows, table):
    logits = dot3(split(rows), table, NN)
    half = 0.5 * jnp.sum(rows * rows, axis=1, keepdims=True)
    return jnp.exp(logits - half) * table[0].shape[1] ** (-0.5)


def pairs_of(refs):
    return [jnp.concatenate([a[...], b[...]], axis=0) for a, b in zip(refs[::2], refs[1::2])]


def key_state(feats, *refs, dh):
    blocks, state = refs[:-1], refs[-1]
    table = split(feats[inner_of(feats.shape[0])])
    total = jnp.zeros((dh, state.shape[1]), F32)
    normal = jnp.zeros((1, state.shape[1]), F32)
    for rows in pairs_of(blocks):
        feat = feats_of(rows[:, :dh], table)
        total = total + dot2(rows[:, dh : 2 * dh].astype(BF16), split(feat), TN)
        normal = normal + jnp.sum(feat, axis=0, keepdims=True)
    state[0:dh] = total
    state[dh:] = jnp.broadcast_to(normal, (state.shape[0] - dh, state.shape[1]))


def both_feats(feats, *refs, dh):
    blocks, (afeat, bfeat) = refs[:-2], refs[-2:]
    table = split(feats[inner_of(feats.shape[0])])
    for i, rows in enumerate(pairs_of(blocks)):
        at = slice(2 * i, 2 * i + 2)
        put(afeat, at, feats_of(rows[:, 2 * dh : 3 * dh], table))
        put(bfeat, at, feats_of(rows[:, :dh], table))


def query_state(afeat, *refs, dh):
    group = afeat.shape[0]
    blocks, parts, (state, scaled, gstate) = refs[:group], refs[group:-3], refs[-3:]
    summed = sum(part[...] for part in parts)
    state[...] = summed
    pair = split(summed)
    total = jnp.zeros(gstate.shape, F32)
    for i, block in enumerate(pairs_of(blocks)):
        at = slice(2 * i, 2 * i + 2)
        upstream = block[:, 3 * dh :]
        feat = split(rows_of(afeat, at))
        both = dot3(feat, pair, NT)
        inv = 1.0 / both[:, dh : dh + 1]
        gn = upstream * inv
        gd = -jnp.sum(gn * both[:, :dh], axis=1, keepdims=True) * inv
        zeros = jnp.zeros((gn.shape[0], gstate.shape[0] - dh - 1), F32)
        rows = jnp.concatenate([gn, gd, zeros], axis=1)
        put(scaled, at, rows)
        total = total + dot3(split(rows), feat, TN)
    gstate[...] = total


def row_grad(rows, feat, grads, table):
    weighted = feat * grads
    back = dot3(split(weighted), table, NT)
    return back - rows * jnp.sum(weighted, axis=1, keepdims=True)


def query_grad(feats, afeat, state, scaled, *refs, dh):
    blocks, out = refs[:-1], refs[-1]
    table = split(feats[inner_of(feats.shape[0])])
    pair = split(state[...])
    for i, rows in enumerate(pairs_of(blocks)):
        at = slice(2 * i, 2 * i + 2)
        grads = dot3(split(rows_of(scaled, at)), pair, NN)
        put(out, at, row_grad(rows[:, 2 * dh : 3 * dh], rows_of(afeat, at), grads, table))


def emit_blocks(outer_index, total, held, outs):
    outer, _, width = held.shape
    for o in range(outer):
        held[o] = total[:, o * width : (o + 1) * width]
    for s, out in enumerate(outs):
        for i in range(out.shape[0]):
            out[i] = held[outer_index ^ (i * len(outs) + s)]


def gather_rows(*refs):
    blocks, rows_all = refs[:-1], refs[-1]
    group = len(blocks) // 2
    half = blocks[0].shape[0]
    inner = inner_of(group)
    for j in range(group):
        start = pl.multiple_of((inner ^ j) * 2 * half, 2 * half)
        for side in range(2):
            rows = blocks[2 * j + side][...].astype(BF16)
            rows_all[pl.ds(start + side * half, half), :] = rows


def key_grad(feats, bfeat, dq, rows_all, *refs, dh, scale, count):
    parts, refs = refs[:count], refs[count:]
    group, tok, _ = bfeat.shape
    keys, out, sents, (left, held) = refs[:group], refs[group], refs[group + 1 : -2], refs[-2:]
    table = split(feats[inner_of(group)])
    summed = sum(part[...] for part in parts)
    pair = split(summed[:dh])
    normal = summed[dh : dh + 1]
    inner = inner_of(group)
    for i, rows in enumerate(pairs_of(keys)):
        at = slice(2 * i, 2 * i + 2)
        grads = dot2(rows[:, dh : 2 * dh].astype(BF16), pair, NN) + normal
        dk = row_grad(rows[:, :dh], rows_of(bfeat, at), grads, table)
        put(out, at, dk)
        both = (jnp.concatenate([rows_of(dq, at), dk], axis=1) * scale).astype(BF16)
        for side in range(2):
            start = pl.multiple_of((inner ^ (2 * i + side)) * tok, tok)
            left[pl.ds(start, tok), :] = both[side * tok : (side + 1) * tok]
    emit_blocks(lax.axis_index("seq") // group, dot1(left[...], rows_all[...], TN), held, sents)


def back_rows(bfeat, dq, dk, *refs, dh, count):
    parts, outs = refs[:count], refs[count:]
    group, tok, _ = bfeat.shape
    pair = split(sum(part[0:dh] for part in parts))
    for i in range(group // 2):
        dv = dot3(split(rows_of(bfeat, slice(2 * i, 2 * i + 2))), pair, NT)
        for side in range(2):
            j = 2 * i + side
            outs[j][0:tok, 0:dh] = dk[j]
            outs[j][0:tok, dh : 2 * dh] = dv[side * tok : (side + 1) * tok]
            outs[j][tok:, 0:dh] = dq[j, 0 : tok // 2]
            outs[j][tok:, dh : 2 * dh] = dq[j, tok // 2 :]


def finish_rows(wq, wk, *refs, scale):
    backs, (grad_hidden, grad_values, back) = refs[:-3], refs[-3:]
    inner = inner_of(len(backs))
    for j, item in enumerate(backs):
        back[inner ^ j] = item[...]
    heads, rows, lanes = back.shape
    tok, dh = rows * 2 // 3, lanes // 2
    dqs, dks = [], []
    for h in range(heads):
        dks.append(back[h, 0:tok, 0:dh])
        dqs.append(jnp.concatenate([back[h, tok:, 0:dh], back[h, tok:, dh:]], axis=0))
        grad_values[:, h * dh : (h + 1) * dh] = back[h, 0:tok, dh:].astype(BF16)
    dq = (jnp.concatenate(dqs, axis=1) * scale).astype(BF16)
    dk = (jnp.concatenate(dks, axis=1) * scale).astype(BF16)
    grad_hidden[...] = dot1(dq, wq[...], NT) + dot1(dk, wk[...], NT)


def turn(*refs, count):
    parts, outs, flat = refs[:count], refs[count:-1], refs[-1]
    turned = sum(part[...] for part in parts).T
    group, rows, _ = flat.shape
    for i in range(group):
        flat[i] = turned[i * rows : (i + 1) * rows]
    inner = inner_of(group)
    for i, out in enumerate(outs):
        for j in range(out.shape[0]):
            out[j] = flat[inner ^ (2 * i + j)]


def join(*refs):
    firsts, last, (gq, gk), own = refs[:-4], refs[-4], refs[-3:-1], refs[-1]
    inner = inner_of(own.shape[0])
    for i, first in enumerate(firsts):
        own[inner ^ (2 * i)] = first[0]
        own[inner ^ (2 * i + 1)] = last[i]
    dh = own.shape[2] // 2
    for h in range(own.shape[0]):
        cols = slice(h * dh, (h + 1) * dh)
        gq[:, cols] = own[h, :, 0:dh]
        gk[:, cols] = own[h, :, dh:]


def make_shards(seq_count, head_count):
    def exchange(value, mask):
        return lax.ppermute(value, "seq", [(i, i ^ mask) for i in range(seq_count)])

    def inner_shards(hidden, query_weight, key_weight, values, grad_out, random_feats):
        tok, width = hidden.shape
        group, dh, feats = random_feats.shape
        outer = seq_count // group
        assert outer * group == seq_count and outer & (outer - 1) == 0
        assert group & (group - 1) == 0 and width % seq_count == 0
        scale = dh ** (-0.25)
        padded = dh + 8
        radices = [2] * ((outer.bit_length() - 1) % 2) + [4] * ((outer.bit_length() - 1) // 2)

        def plane_parts(value):
            parts, stride = [value], group
            for radix in radices:
                value = sum(parts)
                parts = [value] + [exchange(value, s * stride) for s in range(1, radix)]
                stride *= radix
            return parts

        def reduce_rows(sent):
            stride = group
            for i, radix in enumerate(radices):
                parts = [sent[0]] + [exchange(sent[s], s * stride) for s in range(1, radix)]
                stride *= radix
                if i + 1 < len(radices):
                    total = sum(parts)
                    total = total.reshape((-1, radices[i + 1]) + total.shape[1:])
                    sent = [total[:, s] for s in range(radices[i + 1])]
            return [part.reshape(part.shape[1:]) for part in parts]

        hbm = pl.BlockSpec(memory_space=pl.ANY)
        vmem = pl.BlockSpec(memory_space=pltpu.VMEM)
        entry = (hidden, key_weight, values, query_weight, grad_out)
        *packed, wide_a, wide_b = pl.pallas_call(
            functools.partial(project, dh=dh, scale=scale),
            out_shape=[pltpu.VMEM((tok, 4 * dh), F32) for _ in range(group)]
            + [pltpu.VMEM((tok // 2, width), F32) for _ in range(2)],
            in_specs=[hbm] * 5,
            out_specs=[vmem] * (group + 2),
            scratch_shapes=[
                pltpu.VMEM((tok, width), BF16),
                pltpu.VMEM((width, group * dh), BF16),
                pltpu.VMEM((width, group * dh), BF16),
                pltpu.VMEM((tok, group * dh), BF16),
                pltpu.VMEM((tok, group * dh), BF16),
                pltpu.VMEM((group, tok, 4 * dh), F32),
                pltpu.SemaphoreType.DMA((11,)),
            ],
            compiler_params=pltpu.CompilerParams(vmem_limit_bytes=LIMIT),
        )(*(pltpu.with_memory_space_constraint(x, pltpu.HBM) for x in entry))
        mine = [packed[0]] + [exchange(item, j) for j, item in enumerate(packed) if j]

        bits = [1 << b for b in range(group.bit_length() - 1)]
        side_a = bits[1:] + bits[:1]
        side_b = bits[1:][::-1] + bits[:1]
        halves = [{0: wide_a}, {0: wide_b}]

        def gather_step(halves, k):
            return [
                side | {j ^ order[k]: exchange(item, order[k]) for j, item in side.items()}
                for side, order in zip(halves, (side_a, side_b))
            ]

        halves = gather_step(halves, 0)
        state = call(
            functools.partial(key_state, dh=dh),
            shape(padded, feats),
            *mine, entry=(random_feats,),
        )
        states = plane_parts(state)
        for k in range(1, len(bits) - 1):
            halves = gather_step(halves, k)
        afeat, bfeat = call(
            functools.partial(both_feats, dh=dh),
            (shape(group, tok, feats), shape(group, tok, feats)),
            *mine, entry=(random_feats,),
        )
        state, scaled, gstate = call(
            functools.partial(query_state, dh=dh),
            (shape(padded, feats), shape(group, tok, padded), shape(padded, feats)),
            afeat, *mine, *states,
        )
        gstates = plane_parts(gstate)
        dq = call(
            functools.partial(query_grad, dh=dh),
            shape(group, tok, dh),
            afeat, state, scaled, *mine, entry=(random_feats,),
        )
        halves = gather_step(halves, len(bits) - 1) if len(bits) > 1 else halves
        blocks = [side[j] for j in range(group) for side in halves]
        rows_all = call(gather_rows, shape(group * tok, width, dtype=BF16), *blocks)
        rows = width // seq_count
        radix = radices[0]
        dk, *sent = call(
            functools.partial(key_grad, dh=dh, scale=scale, count=len(gstates)),
            (shape(group, tok, dh),)
            + tuple(shape(outer // radix, 2 * dh, width // outer) for _ in range(radix)),
            bfeat, dq, rows_all, *gstates, *mine, entry=(random_feats,),
            scratch=[
                pltpu.VMEM((group * tok, 2 * dh), BF16),
                pltpu.VMEM((outer, 2 * dh, width // outer), F32),
            ],
        )
        parts = reduce_rows(sent)
        backs = call(
            functools.partial(back_rows, dh=dh, count=len(gstates)),
            tuple(shape(tok + tok // 2, 2 * dh) for _ in range(group)),
            bfeat, dq, dk, *gstates,
        )
        backs = [backs[0]] + [exchange(item, j) for j, item in enumerate(backs) if j]
        grad_hidden, grad_values = call(
            functools.partial(finish_rows, scale=scale),
            (shape(tok, width), shape(tok, group * dh, dtype=BF16)),
            *backs, entry=(query_weight, key_weight), final=True,
            scratch=[pltpu.VMEM((group, tok + tok // 2, 2 * dh), F32)],
        )
        if head_count > 1:
            grad_hidden = lax.psum(grad_hidden, "head")
        mine, *others = call(
            functools.partial(turn, count=len(parts)),
            tuple(shape(2, rows, 2 * dh) for _ in range(group // 2)),
            *parts,
            scratch=[pltpu.VMEM((group, rows, 2 * dh), F32)],
        )
        firsts = [mine] + [exchange(item, 2 * i + 2) for i, item in enumerate(others)]
        last = exchange(jnp.stack([item[1] for item in firsts]), 1)
        grad_query_weight, grad_key_weight = call(
            join, (shape(rows, group * dh), shape(rows, group * dh)),
            *firsts, last, final=True,
            scratch=[pltpu.VMEM((group, rows, 2 * dh), F32)],
        )
        return (grad_hidden, grad_values, grad_query_weight, grad_key_weight)

    return inner_shards


def solution(mesh):
    placed = (
        P("seq", None),
        P(None, "head"),
        P(None, "head"),
        P("seq", "head"),
        P("seq", "head"),
        P("head", None, None),
    )
    return jax.shard_map(
        make_shards(mesh.shape["seq"], mesh.shape["head"]),
        mesh=mesh,
        in_specs=placed,
        out_specs=(P("seq", None), P("seq", "head"), P("seq", "head"), P("seq", "head")),
        check_vma=False,
    )
```
